256 devices in a mesh: replica: 8 (over y, x_lo), fsdp: 32 (over z, x_hi, core).
Axes of the slice: x: 4 (x_hi: 2, x_lo: 2; x = x_hi * 2 + x_lo), y: 4, z: 8, core: 2. Of those that a mesh axis runs over, the one named last changes fastest.
Arguments:
- local_weights: bfloat16 [8, 1024, 28672], P('replica', 'fsdp'), may hold values from -6 to 6
- base_weights: float32 [1024, 28672], P('fsdp'), may hold values from -6 to 6
- momentum: float32 [1024, 28672], P('replica', 'fsdp'), may hold values from -4 to 4
Outputs:
- new_weights: float32 [1024, 28672], P('fsdp')
- new_momentum: float32 [1024, 28672], P('replica', 'fsdp')
The draws below stay inside these ranges and needn't reach their ends.
All inputs are finite; a program needn't handle non-finite values. Where the reference program divides by a largest or mean magnitude, that divisor is 1e-20 or more.
Results may differ from the reference program's by a relative error of at most 0.015.
Values may be sent and summed in bfloat16 or wider, within the bound.
No kernel may reach another device: no remote copies, remote signals or barrier semaphores. Data moves between devices by JAX's collectives and lax.ppermute only.
A program may use at most 128 MiB of HBM per device.

```python
import jax
import jax.numpy as jnp

FF = 28672
QBLOCK = 128
REPLICAS = 8
ROWS = 1024


def block_levels(rng, shape, shards, smallest, top_value):
    level, own = 1.0, jax.random.fold_in(rng, 6)
    for dim, shards_of in shards:
        steps = jnp.exp(jax.random.uniform(jax.random.fold_in(own, dim), (shards_of,), jnp.float32, smallest / len(shards), top_value / len(shards)))
        level = level * jnp.repeat(steps, shape[dim] // shards_of).reshape([-1 if axis == dim else 1 for axis in range(len(shape))])
    return level


def gaussian(key, dims, spread, most, split=(), dtype=jnp.bfloat16):
    drawn = spread * jax.random.normal(key, dims, jnp.float32)
    if split:
        drawn = drawn * block_levels(key, dims, split, -0.22, 0.18)
    return jnp.clip(drawn, -most, most).astype(dtype)


def setup_inputs(seed: int = 0) -> dict:
    seeds = jax.random.split(jax.random.key(seed), 4)
    return {
        "local_weights": gaussian(seeds[0], (REPLICAS, ROWS, FF), 1.0, 6.0, ((0, 8), (1, 32))),
        "base_weights": gaussian(seeds[1], (ROWS, FF), 1.0, 6.0, ((0, 32),), jnp.float32),
        "momentum": gaussian(seeds[2], (ROWS, FF), 0.5, 4.0, ((0, 8), (1, 32)), jnp.float32),
    }


EPSILON = 1e-6
LEARN_RATE = 0.7
MOMENTUM_COEF = 0.9


def block_quantize(replica_differences):
    row_count = replica_differences.shape[0]
    block_grouped = replica_differences.reshape(row_count, -1, QBLOCK)
    block_scales = (jnp.max(jnp.abs(block_grouped), axis=2) + EPSILON).astype(jnp.bfloat16)
    integer_levels = (block_grouped / block_scales.astype(jnp.float32)[:, :, None]).astype(jnp.bfloat16)
    return integer_levels, block_scales


def reference(local_weights, base_weights, momentum):
    total = jnp.zeros(base_weights.shape, jnp.float32)
    for replica in range(REPLICAS):
        replica_differences = base_weights - local_weights[replica].astype(jnp.float32)
        integer_levels, block_scales = block_quantize(replica_differences)
        values = integer_levels.astype(jnp.float32) * block_scales.astype(jnp.float32)[:, :, None]
        total = total + values.reshape(base_weights.shape)
    average = total / REPLICAS
    new_momentum = MOMENTUM_COEF * momentum + average
    update = (LEARN_RATE * (average + MOMENTUM_COEF * new_momentum)).astype(jnp.bfloat16)
    new_weights = base_weights - update.astype(jnp.float32)
    return new_weights, new_momentum
```

```python
import jax
import jax.numpy as jnp
from jax import lax
from jax.experimental import pallas as pl
from jax.experimental.pallas import tpu as pltpu
from jax.sharding import Mesh
from jax.sharding import PartitionSpec as P

R = ("y", "xl")
J = ("xh", "c")
FSDP = ("z", "xh", "c")
LEARN_RATE = 0.7
MOMENTUM_COEF = 0.9
CHUNKS = 2


def delta_parts(local, base, z, chunk, width):
    rows = base.shape[0]
    count = local.shape[1] // (CHUNKS * width)

    def body(z_ref, local_ref, base_ref, out_ref):
        out_ref[...] = (base_ref[...] - local_ref[...].astype(jnp.float32)).astype(jnp.bfloat16)

    def block(r, z_ref):
        return (0, CHUNKS * (r ^ z_ref[0]) + chunk)

    return pl.pallas_call(
        body,
        grid_spec=pltpu.PrefetchScalarGridSpec(
            num_scalar_prefetch=1,
            grid=(count,),
            in_specs=[pl.BlockSpec((rows, width), block), pl.BlockSpec((rows, width), block)],
            out_specs=pl.BlockSpec((None, rows, width), lambda r, z_ref: (r, 0, 0)),
        ),
        out_shape=jax.ShapeDtypeStruct((count, rows, width), jnp.bfloat16),
        name=f"delta_{chunk}",
    )(z, local, base)


def sum_update(parts, momentum, chunk):
    count, rows, width = parts.shape
    pieces, _, inner = momentum.shape
    mine = pieces // CHUNKS

    def body(parts_ref, m_ref, out_ref, avg_ref):
        for p in range(mine):
            for k in range(0, inner, 128):
                col = p * inner + k
                total = parts_ref[0, :, col : col + 128].astype(jnp.float32)
                for r in range(1, count):
                    total = total + parts_ref[r, :, col : col + 128].astype(jnp.float32)
                average = total * (1.0 / count)
                old = m_ref[chunk * mine + p, :, k : k + 128].astype(jnp.float32)
                new = MOMENTUM_COEF * old + average
                update = (LEARN_RATE * (average + MOMENTUM_COEF * new)).astype(jnp.bfloat16)
                avg_ref[p, :, k : k + 128] = average.astype(jnp.bfloat16)
                for r in range(count):
                    out_ref[r, :, col : col + 128] = update

    return pl.pallas_call(
        body,
        in_specs=[pl.BlockSpec(memory_space=pltpu.VMEM)] * 2,
        out_specs=[pl.BlockSpec(memory_space=pltpu.VMEM)] * 2,
        out_shape=[
            jax.ShapeDtypeStruct(parts.shape, jnp.bfloat16),
            jax.ShapeDtypeStruct((mine, rows, inner), jnp.bfloat16),
        ],
        name=f"update_{chunk}",
    )(parts, momentum)


def apply_update(base, parts, z, chunk, earlier):
    count, rows, width = parts.shape

    def body(z_ref, base_ref, part_ref, *refs):
        refs[-1][...] = base_ref[...] - part_ref[...].astype(jnp.float32)

    def block(r, z_ref):
        return (0, CHUNKS * (r ^ z_ref[0]) + chunk)

    more = [] if earlier is None else [earlier]
    return pl.pallas_call(
        body,
        grid_spec=pltpu.PrefetchScalarGridSpec(
            num_scalar_prefetch=1,
            grid=(count,),
            in_specs=[
                pl.BlockSpec((rows, width), block),
                pl.BlockSpec((None, rows, width), lambda r, z_ref: (r, 0, 0)),
            ]
            + [pl.BlockSpec(memory_space=pl.ANY)] * len(more),
            out_specs=pl.BlockSpec((rows, width), block),
        ),
        out_shape=jax.ShapeDtypeStruct(base.shape, base.dtype),
        input_output_aliases={3: 0} if more else {},
        name=f"apply_{chunk}",
    )(z, base, parts, *more)


def per_device(local_weights, base_weights, momentum):
    count = lax.axis_size(R)
    rows, cols = base_weights.shape
    width = cols // (count * CHUNKS)
    z = lax.axis_index("z").reshape(1)
    local = local_weights[0]
    there = [(r * count + p, (r ^ p) * count + r) for r in range(count) for p in range(count)]
    back = [(b, a) for a, b in there]
    pieces = lax.axis_size(J)

    summed = []
    for c in range(CHUNKS):
        parts = delta_parts(local, base_weights, z, c, width)
        summed.append(lax.all_to_all(parts, R, 0, 0, tiled=True))
        if c == 0:
            m = momentum.astype(jnp.bfloat16).reshape(pieces, rows, -1)
            m = lax.all_to_all(m, J, 0, 0, tiled=True)
            m = lax.ppermute(m, R + ("z",), there)
    averages, updates = [], []
    for c in range(CHUNKS):
        copies, average = sum_update(summed[c], m, c)
        averages.append(average)
        updates.append(lax.all_to_all(copies, R, 0, 0, tiled=True))
    average = lax.ppermute(jnp.concatenate(averages), R + ("z",), back)
    average = lax.all_to_all(average, J, 0, 0, tiled=True)
    new_momentum = MOMENTUM_COEF * momentum + average.reshape(momentum.shape).astype(jnp.float32)
    new_weights = None
    for c in range(CHUNKS):
        new_weights = apply_update(base_weights, updates[c], z, c, new_weights)
    return new_weights, new_momentum


def solution(mesh):
    finer = Mesh(mesh.devices.reshape(4, 2, 8, 2, 2), ("y", "xl", "z", "xh", "c"))
    in_specs = (P(R, FSDP, None), P(FSDP, None), P(R, FSDP))
    out_specs = (P(FSDP, None), P(R, FSDP))
    return jax.shard_map(per_device, mesh=finer, in_specs=in_specs, out_specs=out_specs, check_vma=False)
```

```python
import jax
import jax.numpy as jnp
import numpy as np
from jax import lax
from jax.experimental import pallas as pl
from jax.experimental.pallas import tpu as pltpu
from jax.sharding import Mesh
from jax.sharding import PartitionSpec as P

R = ("y", "xl")
FSDP = ("z", "xh", "c")
EVERY = R + FSDP
LEARN_RATE = 0.7
MOMENTUM_COEF = 0.9
HALF = 16
WIDE = 896

MASKS = {"x": 1, "a": 2, "b": 6}
PARTS = (("xab", (0, 1, 2)), ("abx", (3, 4, 5)), ("bxa", (6, 7)))


def column_plane(r, z, c):
    return r ^ z ^ (7 * c)


def device(r, z, xh, c):
    return ((r * 8 + z) * 2 + xh) * 2 + c


def pairs(there):
    found = []
    for r in range(8):
        for z in range(8):
            for xh in range(2):
                for c in range(2):
                    found.append((device(r, z, xh, c), device(*there(r, z, xh, c))))
    return found


def send(value, there):
    return lax.ppermute(value, EVERY, pairs(there))


def exchange(value, dim):
    return send(value, lambda r, z, xh, c: (r ^ MASKS[dim], z, xh, c))


def peer(order, first, second, third):
    return (first * MASKS[order[0]]) ^ (second * MASKS[order[1]]) ^ (third * MASKS[order[2]])


def blocks_of(half):
    listed = []
    for p, (order, units) in enumerate(PARTS):
        for second in range(2):
            for third in range(2):
                for n, unit in enumerate(units):
                    listed.append((p, (second * 2 + third, n), peer(order, half, second, third), unit))
    return listed


def place_of(peer_index, unit):
    r = lax.axis_index(R) ^ peer_index
    z, xh, c = lax.axis_index("z"), lax.axis_index("xh"), lax.axis_index("c")
    core = c ^ (unit // 4)
    column = 4 * column_plane(r, z, core) + 2 * (xh ^ (unit // 2 % 2)) + core
    return HALF * (unit % 2), pl.multiple_of(column * WIDE, 128)


def shapes_of():
    return [(4, len(units), HALF, WIDE) for _, units in PARTS]


def deltas(local, base, half):
    blocks = blocks_of(half)

    def body(local_hbm, base_hbm, *refs):
        outs, (local_buf, base_buf, local_sem, base_sem) = refs[:3], refs[3:]
        copies = []
        for n, (_, _, k, unit) in enumerate(blocks):
            row, col = place_of(k, unit)
            here = (pl.ds(row, HALF), pl.ds(col, WIDE))
            one = pltpu.make_async_copy(base_hbm.at[here], base_buf.at[n], base_sem.at[n])
            two = pltpu.make_async_copy(local_hbm.at[here], local_buf.at[n], local_sem.at[n])
            one.start()
            two.start()
            copies.append((one, two))
        for n, (p, at, _, _) in enumerate(blocks):
            for copy in copies[n]:
                copy.wait()
            outs[p][at] = (base_buf[n] - local_buf[n].astype(jnp.float32)).astype(jnp.bfloat16)

    return pl.pallas_call(
        body,
        in_specs=[pl.BlockSpec(memory_space=pl.ANY)] * 2,
        out_specs=[pl.BlockSpec(memory_space=pltpu.VMEM)] * 3,
        out_shape=[jax.ShapeDtypeStruct(s, jnp.bfloat16) for s in shapes_of()],
        scratch_shapes=[
            pltpu.VMEM((len(blocks), HALF, WIDE), jnp.bfloat16),
            pltpu.VMEM((len(blocks), HALF, WIDE), jnp.float32),
            pltpu.SemaphoreType.DMA((len(blocks),)),
            pltpu.SemaphoreType.DMA((len(blocks),)),
        ],
        name=f"delta_{half}",
    )(local, base)


def apply_updates(base, updates, half, earlier):
    blocks = blocks_of(half)

    def body(base_hbm, *refs):
        parts, out_hbm = refs[:3], refs[-5]
        base_buf, out_buf, base_sem, out_sem = refs[-4:]
        copies = []
        for n, (_, _, k, unit) in enumerate(blocks):
            row, col = place_of(k, unit)
            here = (pl.ds(row, HALF), pl.ds(col, WIDE))
            one = pltpu.make_async_copy(base_hbm.at[here], base_buf.at[n], base_sem.at[n])
            two = pltpu.make_async_copy(out_buf.at[n], out_hbm.at[here], out_sem.at[n])
            one.start()
            copies.append((one, two))
        for n, (p, at, _, _) in enumerate(blocks):
            copies[n][0].wait()
            out_buf[n] = base_buf[n] - parts[p][at].astype(jnp.float32)
            copies[n][1].start()
        for n in range(len(blocks)):
            copies[n][1].wait()

    more = [] if earlier is None else [earlier]
    return pl.pallas_call(
        body,
        in_specs=[pl.BlockSpec(memory_space=pl.ANY)]
        + [pl.BlockSpec(memory_space=pltpu.VMEM)] * 3
        + [pl.BlockSpec(memory_space=pl.ANY)] * len(more),
        out_specs=pl.BlockSpec(memory_space=pl.ANY),
        out_shape=jax.ShapeDtypeStruct(base.shape, base.dtype),
        input_output_aliases={4: 0} if more else {},
        scratch_shapes=[
            pltpu.VMEM((len(blocks), HALF, WIDE), jnp.float32),
            pltpu.VMEM((len(blocks), HALF, WIDE), jnp.float32),
            pltpu.SemaphoreType.DMA((len(blocks),)),
            pltpu.SemaphoreType.DMA((len(blocks),)),
        ],
        name=f"apply_{half}",
    )(base, *updates, *more)


def turned(value, axis, dim):
    return jnp.where(lax.axis_index(axis) == 0, value, jnp.flip(value, dim))


def momentum_to_holders(momentum):
    rows = 2 * HALF
    m = momentum.astype(jnp.bfloat16).reshape(2, 2, rows, WIDE)
    m = turned(turned(m, "xh", 0), "c", 1)
    holder = {(column_plane(r, z, c), z, c): r for r in range(8) for z in range(8) for c in range(2)}
    moved = [send(m[dx], lambda r, z, xh, c: (holder[z, r, c], z, xh ^ dx, c)) for dx in range(2)]
    owner = {(r, column_plane(r, z, c), c): z for r in range(8) for z in range(8) for c in range(2)}
    m = send(jnp.stack(moved), lambda r, z, xh, c: (r, owner[r, z, c], xh, c))
    other = send(m[:, 1], lambda r, z, xh, c: (r, z, xh, 1 - c))
    return jnp.stack([m[:, 0], other]).reshape(8, HALF, WIDE)


def average_to_owners(average):
    average = average.reshape(2, 2, 2 * HALF, WIDE)
    other = send(average[1], lambda r, z, xh, c: (r, z, xh, 1 - c))
    moved = [
        send(
            jnp.stack([average[0, dx], other[dx]]),
            lambda r, z, xh, c: (z, column_plane(r, z, c), xh ^ dx, c),
        )
        for dx in range(2)
    ]
    return turned(turned(jnp.stack(moved), "c", 1), "xh", 0)


def per_device(local_weights, base_weights, momentum):
    count = lax.axis_size(R)
    local = local_weights[0]
    sums = list(deltas(local, base_weights, 1))
    held = momentum_to_holders(momentum)
    got = [exchange(sums[p], order[0]) for p, (order, _) in enumerate(PARTS)]
    kept = deltas(local, base_weights, 0)
    f32 = lambda v: v.astype(jnp.float32)
    total, averages, updates = [], [], []
    for p, (order, units) in enumerate(PARTS):
        total.append((f32(kept[p]) + f32(got[p])).reshape(2, 2, *kept[p].shape[1:]))
    for p, (order, units) in enumerate(PARTS):
        got[p] = exchange(total[p][1].astype(jnp.bfloat16), order[1])
    for p, (order, units) in enumerate(PARTS):
        total[p] = total[p][0] + f32(got[p])
        got[p] = exchange(total[p][1].astype(jnp.bfloat16), order[2])
    for p, (order, units) in enumerate(PARTS):
        average = (total[p][0] + f32(got[p])) * (1.0 / count)
        new = MOMENTUM_COEF * f32(held[units[0] : units[-1] + 1]) + average
        averages.append(average.astype(jnp.bfloat16))
        updates.append((LEARN_RATE * (average + MOMENTUM_COEF * new)).astype(jnp.bfloat16)[None])
    for p, (order, units) in enumerate(PARTS):
        updates[p] = jnp.concatenate([updates[p], exchange(updates[p], order[2])])
    returned = average_to_owners(jnp.concatenate(averages))
    for p, (order, units) in enumerate(PARTS):
        updates[p] = jnp.concatenate([updates[p], exchange(updates[p], order[1])])
    last = [exchange(updates[p], order[0]) for p, (order, _) in enumerate(PARTS)]
    new_momentum = MOMENTUM_COEF * momentum + f32(returned).reshape(momentum.shape)
    new_weights = apply_updates(base_weights, updates, 0, None)
    new_weights = apply_updates(base_weights, last, 1, new_weights)
    return new_weights, new_momentum


def solution(mesh):
    finer = Mesh(mesh.devices.reshape(4, 2, 8, 2, 2), EVERY)
    in_specs = (P(R, FSDP, None), P(FSDP, None), P(R, FSDP))
    out_specs = (P(FSDP, None), P(R, FSDP))
    return jax.shard_map(per_device, mesh=finer, in_specs=in_specs, out_specs=out_specs, check_vma=False)
```

```python
import jax
import jax.numpy as jnp
from jax import lax
from jax.experimental import pallas as pl
from jax.experimental.pallas import tpu as pltpu
from jax.sharding import Mesh
from jax.sharding import PartitionSpec as P


R = ("y", "xl")
FSDP = ("z", "xh", "c")
EVERY = R + FSDP
LEARN_RATE = 0.7
MOMENTUM_COEF = 0.9
HALF = 16
WIDE = 896
VMEM_LIMIT = 12 << 20

MASKS = {"x": 1, "a": 2, "b": 6}
PARTS = (("xab", (0, 1, 2)), ("abx", (3, 4, 5)), ("bxa", (6, 7)))


def column_plane(r, z, c):
    return r ^ z ^ (7 * c)


def device(r, z, xh, c):
    return ((r * 8 + z) * 2 + xh) * 2 + c


def pairs(there):
    found = []
    for r in range(8):
        for z in range(8):
            for xh in range(2):
                for c in range(2):
                    found.append((device(r, z, xh, c), device(*there(r, z, xh, c))))
    return found


def send(value, there):
    return lax.ppermute(value, EVERY, pairs(there))


def exchange(value, dim):
    return send(value, lambda r, z, xh, c: (r ^ MASKS[dim], z, xh, c))


def in_vmem(value):
    return pltpu.with_memory_space_constraint(value, pltpu.VMEM)


def peer(order, first, second, third):
    return (first * MASKS[order[0]]) ^ (second * MASKS[order[1]]) ^ (third * MASKS[order[2]])


def blocks_of(half):
    listed = []
    for p, (order, units) in enumerate(PARTS):
        for second in range(2):
            for third in range(2):
                for n, unit in enumerate(units):
                    listed.append((p, (second * 2 + third, n), peer(order, half, second, third), unit))
    return listed


def place_of(peer_index, unit):
    r = lax.axis_index(R) ^ peer_index
    z, xh, c = lax.axis_index("z"), lax.axis_index("xh"), lax.axis_index("c")
    core = c ^ (unit // 4)
    column = 4 * column_plane(r, z, core) + 2 * (xh ^ (unit // 2 % 2)) + core
    return HALF * (unit % 2), pl.multiple_of(column * WIDE, 128)


def shapes_of():
    return [(4, len(units), HALF, WIDE) for _, units in PARTS]


def deltas(local, base, momentum, half):
    blocks = blocks_of(half)
    count = len(blocks)
    lead = 2 if momentum is not None else 0
    rows = 2 * HALF

    def body(*refs):
        local_hbm, base_hbm, *refs = refs
        if lead:
            old_hbm, *refs = refs
        outs, base_buf, refs = refs[:3], refs[3], refs[4:]
        if lead:
            moved, old_buf, refs = refs[:2], refs[2], refs[3:]
        local_buf, local_sem, base_sem = refs[:3]
        copies = []
        for n, (_, _, k, unit) in enumerate(blocks):
            row, col = place_of(k, unit)
            here = (pl.ds(row, HALF), pl.ds(col, WIDE))
            one = pltpu.make_async_copy(base_hbm.at[here], base_buf.at[n], base_sem.at[n])
            two = pltpu.make_async_copy(local_hbm.at[here], local_buf.at[n], local_sem.at[n])
            one.start()
            two.start()
            copies.append((one, two))
        if lead:
            old_sem = refs[3]
            xh, c = lax.axis_index("xh"), lax.axis_index("c")
            old_copies = []
            for dx in range(2):
                for dc in range(2):
                    row = pl.multiple_of(rows * (2 * (xh ^ dx) + (c ^ dc)), rows)
                    copy = pltpu.make_async_copy(
                        old_hbm.at[pl.ds(row, rows)], old_buf.at[dx, dc], old_sem.at[dx, dc]
                    )
                    copy.start()
                    old_copies.append((dx, dc, copy))
        for n, (p, at, _, _) in enumerate(blocks):
            for copy in copies[n]:
                copy.wait()
            outs[p][at] = (base_buf[n] - local_buf[n].astype(jnp.float32)).astype(jnp.bfloat16)
        if lead:
            for dx, dc, copy in old_copies:
                copy.wait()
                moved[dx][dc] = old_buf[dx, dc].astype(jnp.bfloat16)

    more = [momentum] if lead else []
    out_shape = [pltpu.VMEM(shape, jnp.bfloat16) for shape in shapes_of()]
    out_shape.append(pltpu.VMEM((count, HALF, WIDE), jnp.float32))
    scratch = [
        pltpu.VMEM((count, HALF, WIDE), jnp.bfloat16),
        pltpu.SemaphoreType.DMA((count,)),
        pltpu.SemaphoreType.DMA((count,)),
    ]
    if lead:
        out_shape += [pltpu.VMEM((2, rows, WIDE), jnp.bfloat16)] * 2
        out_shape.append(pltpu.VMEM((2, 2, rows, WIDE), jnp.float32))
        scratch.append(pltpu.SemaphoreType.DMA((2, 2)))
    return pl.pallas_call(
        body,
        in_specs=[pl.BlockSpec(memory_space=pltpu.HBM)] * (2 + len(more)),
        out_specs=[pl.BlockSpec(memory_space=pltpu.VMEM)] * len(out_shape),
        out_shape=out_shape,
        scratch_shapes=scratch,
        compiler_params=pltpu.CompilerParams(vmem_limit_bytes=VMEM_LIMIT),
    )(*[pltpu.with_memory_space_constraint(v, pltpu.HBM) for v in (local, base, *more)])


def apply_updates(base_blocks, updates, half, shape, earlier):
    blocks = blocks_of(half)

    def body(base_buf, *refs):
        parts, out_hbm, out_buf, out_sem = refs[:3], refs[-3], refs[-2], refs[-1]
        copies = []
        for n, (p, at, k, unit) in enumerate(blocks):
            row, col = place_of(k, unit)
            out_buf[n] = base_buf[n] - parts[p][at].astype(jnp.float32)
            there = out_hbm.at[pl.ds(row, HALF), pl.ds(col, WIDE)]
            copy = pltpu.make_async_copy(out_buf.at[n], there, out_sem.at[n])
            copy.start()
            copies.append(copy)
        for copy in copies:
            copy.wait()

    more = [] if earlier is None else [earlier]
    return pl.pallas_call(
        body,
        in_specs=[pl.BlockSpec(memory_space=pltpu.VMEM)] * 4
        + [pl.BlockSpec(memory_space=pltpu.HBM)] * len(more),
        out_specs=pl.BlockSpec(memory_space=pltpu.HBM),
        out_shape=jax.ShapeDtypeStruct(shape, jnp.float32),
        input_output_aliases={4: 0} if more else {},
        scratch_shapes=[
            pltpu.VMEM((len(blocks), HALF, WIDE), jnp.float32),
            pltpu.SemaphoreType.DMA((len(blocks),)),
        ],
        compiler_params=pltpu.CompilerParams(vmem_limit_bytes=VMEM_LIMIT),
    )(in_vmem(base_blocks), *[in_vmem(u) for u in updates], *more)


def next_momentum(old, returned, shape):
    rows = 2 * HALF

    def body(old_buf, *refs):
        pieces, out_hbm, out_buf, out_sem = refs[:2], refs[2], refs[3], refs[4]
        xh, c = lax.axis_index("xh"), lax.axis_index("c")
        copies = []
        for dx in range(2):
            for dc in range(2):
                row = pl.multiple_of(rows * (2 * (xh ^ dx) + (c ^ dc)), rows)
                out_buf[dx, dc] = MOMENTUM_COEF * old_buf[dx, dc] + pieces[dx][dc].astype(jnp.float32)
                copy = pltpu.make_async_copy(
                    out_buf.at[dx, dc], out_hbm.at[pl.ds(row, rows)], out_sem.at[dx, dc]
                )
                copy.start()
                copies.append(copy)
        for copy in copies:
            copy.wait()

    return pl.pallas_call(
        body,
        in_specs=[pl.BlockSpec(memory_space=pltpu.VMEM)] * 3,
        out_specs=pl.BlockSpec(memory_space=pltpu.HBM),
        out_shape=jax.ShapeDtypeStruct(shape, jnp.float32),
        scratch_shapes=[pltpu.VMEM(old.shape, jnp.float32), pltpu.SemaphoreType.DMA((2, 2))],
        compiler_params=pltpu.CompilerParams(vmem_limit_bytes=VMEM_LIMIT),
        name="momentum",
    )(in_vmem(old), *[in_vmem(v) for v in returned])


def momentum_to_holders(m):
    holder = {(column_plane(r, z, c), z, c): r for r in range(8) for z in range(8) for c in range(2)}
    moved = [send(m[dx], lambda r, z, xh, c: (holder[z, r, c], z, xh ^ dx, c)) for dx in range(2)]
    owner = {(r, column_plane(r, z, c), c): z for r in range(8) for z in range(8) for c in range(2)}
    m = send(jnp.stack(moved), lambda r, z, xh, c: (r, owner[r, z, c], xh, c))
    other = send(m[:, 1], lambda r, z, xh, c: (r, z, xh, 1 - c))
    return jnp.stack([m[:, 0], other]).reshape(8, HALF, WIDE)


def average_to_owners(average):
    average = average.reshape(2, 2, 2 * HALF, WIDE)
    other = send(average[1], lambda r, z, xh, c: (r, z, xh, 1 - c))
    return [
        send(
            jnp.stack([average[0, dx], other[dx]]),
            lambda r, z, xh, c: (z, column_plane(r, z, c), xh ^ dx, c),
        )
        for dx in range(2)
    ]


def f32(value):
    return value.astype(jnp.float32)


def b16(value):
    return value.astype(jnp.bfloat16)


def per_device(local_weights, base_weights, momentum):
    return outer_step(local_weights[0], base_weights, momentum)


def outer_step(local, base, momentum):
    count = lax.axis_size(R)
    *sends, base_1, m_0, m_1, old = deltas(local, base, momentum, 1)
    held = momentum_to_holders([m_0, m_1])
    first = [exchange(sends[p], order[0]) for p, (order, _) in enumerate(PARTS)]
    *kept, base_0 = deltas(local, base, None, 0)
    second, third, averages, updates = [], [], [], []
    for p, (order, units) in enumerate(PARTS):
        out = b16(f32(kept[p][2:]) + f32(first[p][2:]))
        second.append(exchange(out, order[1]))
    for p, (order, units) in enumerate(PARTS):
        out = b16(f32(kept[p][1]) + f32(first[p][1]) + f32(second[p][1]))
        third.append(exchange(out, order[2]))
    for p, (order, units) in enumerate(PARTS):
        total = f32(kept[p][0]) + f32(first[p][0]) + f32(second[p][0]) + f32(third[p])
        average = total * (1.0 / count)
        new = MOMENTUM_COEF * f32(held[units[0] : units[-1] + 1]) + average
        averages.append(b16(average))
        updates.append(b16(LEARN_RATE * (average + MOMENTUM_COEF * new))[None])
    returned = average_to_owners(jnp.concatenate(averages))
    for step in (2, 1):
        for p, (order, units) in enumerate(PARTS):
            more = exchange(updates[p], order[step])
            updates[p] = jnp.concatenate([updates[p], more])
    last = [exchange(updates[p], order[0]) for p, (order, _) in enumerate(PARTS)]
    new_weights = apply_updates(base_0, updates, 0, base.shape, None)
    new_momentum = next_momentum(old, returned, momentum.shape)
    new_weights = apply_updates(base_1, last, 1, base.shape, new_weights)
    return new_weights, new_momentum


def solution(mesh):
    finer = Mesh(mesh.devices.reshape(4, 2, 8, 2, 2), EVERY)
    in_specs = (P(R, FSDP, None), P(FSDP, None), P(R, FSDP))
    out_specs = (P(FSDP, None), P(R, FSDP))
    return jax.shard_map(per_device, mesh=finer, in_specs=in_specs, out_specs=out_specs, check_vma=False)
```

```python
import jax
import jax.numpy as jnp
from jax import lax
from jax.experimental import pallas as pl
from jax.experimental.pallas import tpu as pltpu
from jax.sharding import Mesh
from jax.sharding import PartitionSpec as P


R = ("y", "xl")
FSDP = ("z", "xh", "c")
EVERY = R + FSDP
LEARN_RATE = 0.7
MOMENTUM_COEF = 0.9
HALF = 16
WIDE = 896
VMEM_LIMIT = 12 << 20

MASKS = {"x": 1, "a": 2, "b": 6}
PARTS = (("xab", (0, 1, 2)), ("abx", (3, 4, 5)), ("bxa", (6, 7)))


def column_plane(r, z, c):
    return r ^ z ^ (5 * c)


def device(r, z, xh, c):
    return ((r * 8 + z) * 2 + xh) * 2 + c


def pairs(there):
    found = []
    for r in range(8):
        for z in range(8):
            for xh in range(2):
                for c in range(2):
                    found.append((device(r, z, xh, c), device(*there(r, z, xh, c))))
    return found


def send(value, there):
    return lax.ppermute(value, EVERY, pairs(there))


def exchange(value, dim):
    return send(value, lambda r, z, xh, c: (r ^ MASKS[dim], z, xh, c))


def in_vmem(value):
    return pltpu.with_memory_space_constraint(value, pltpu.VMEM)


def peer(order, first, second, third):
    return (first * MASKS[order[0]]) ^ (second * MASKS[order[1]]) ^ (third * MASKS[order[2]])


def blocks_of(half):
    listed = []
    for p, (order, units) in enumerate(PARTS):
        for second in range(2):
            for third in range(2):
                for n, unit in enumerate(units):
                    listed.append((p, (second * 2 + third, n), peer(order, half, second, third), unit))
    return listed


def place_of(peer_index, unit):
    r = lax.axis_index(R) ^ peer_index
    z, xh, c = lax.axis_index("z"), lax.axis_index("xh"), lax.axis_index("c")
    column = 4 * column_plane(r, z, c) + 2 * (xh ^ (unit // 4)) + (c ^ (unit // 2 % 2))
    return HALF * (unit % 2), pl.multiple_of(column * WIDE, 128)


def shapes_of():
    return [(4, len(units), HALF, WIDE) for _, units in PARTS]


def deltas(local, base, momentum, half):
    blocks = blocks_of(half)
    count = len(blocks)
    lead = 2 if momentum is not None else 0
    rows = 2 * HALF

    def body(*refs):
        local_hbm, base_hbm, *refs = refs
        if lead:
            old_hbm, *refs = refs
        outs, base_buf, refs = refs[:3], refs[3], refs[4:]
        if lead:
            moved, old_buf, refs = refs[:2], refs[2], refs[3:]
        local_buf, local_sem, base_sem = refs[:3]
        copies = []
        for n, (_, _, k, unit) in enumerate(blocks):
            row, col = place_of(k, unit)
            here = (pl.ds(row, HALF), pl.ds(col, WIDE))
            one = pltpu.make_async_copy(base_hbm.at[here], base_buf.at[n], base_sem.at[n])
            two = pltpu.make_async_copy(local_hbm.at[here], local_buf.at[n], local_sem.at[n])
            one.start()
            two.start()
            copies.append((one, two))
        if lead:
            old_sem = refs[3]
            xh, c = lax.axis_index("xh"), lax.axis_index("c")
            old_copies = []
            for dx in range(2):
                for dc in range(2):
                    row = pl.multiple_of(rows * (2 * (xh ^ dx) + (c ^ dc)), rows)
                    copy = pltpu.make_async_copy(
                        old_hbm.at[pl.ds(row, rows)], old_buf.at[dx, dc], old_sem.at[dx, dc]
                    )
                    copy.start()
                    old_copies.append((dx, dc, copy))
        for n, (p, at, _, _) in enumerate(blocks):
            for copy in copies[n]:
                copy.wait()
            outs[p][at] = (base_buf[n] - local_buf[n].astype(jnp.float32)).astype(jnp.bfloat16)
        if lead:
            for dx, dc, copy in old_copies:
                copy.wait()
                moved[dc][dx] = old_buf[dx, dc].astype(jnp.bfloat16)

    more = [momentum] if lead else []
    out_shape = [pltpu.VMEM(shape, jnp.bfloat16) for shape in shapes_of()]
    out_shape.append(pltpu.VMEM((count, HALF, WIDE), jnp.float32))
    scratch = [
        pltpu.VMEM((count, HALF, WIDE), jnp.bfloat16),
        pltpu.SemaphoreType.DMA((count,)),
        pltpu.SemaphoreType.DMA((count,)),
    ]
    if lead:
        out_shape += [pltpu.VMEM((2, rows, WIDE), jnp.bfloat16)] * 2
        out_shape.append(pltpu.VMEM((2, 2, rows, WIDE), jnp.float32))
        scratch.append(pltpu.SemaphoreType.DMA((2, 2)))
    return pl.pallas_call(
        body,
        in_specs=[pl.BlockSpec(memory_space=pltpu.HBM)] * (2 + len(more)),
        out_specs=[pl.BlockSpec(memory_space=pltpu.VMEM)] * len(out_shape),
        out_shape=out_shape,
        scratch_shapes=scratch,
        compiler_params=pltpu.CompilerParams(vmem_limit_bytes=VMEM_LIMIT),
    )(*[pltpu.with_memory_space_constraint(v, pltpu.HBM) for v in (local, base, *more)])


def apply_updates(base_blocks, updates, half, shape, earlier):
    blocks = blocks_of(half)

    def body(base_buf, *refs):
        parts, out_hbm, out_buf, out_sem = refs[:3], refs[-3], refs[-2], refs[-1]
        copies = []
        for n, (p, at, k, unit) in enumerate(blocks):
            row, col = place_of(k, unit)
            out_buf[n] = base_buf[n] - parts[p][at].astype(jnp.float32)
            there = out_hbm.at[pl.ds(row, HALF), pl.ds(col, WIDE)]
            copy = pltpu.make_async_copy(out_buf.at[n], there, out_sem.at[n])
            copy.start()
            copies.append(copy)
        for copy in copies:
            copy.wait()

    more = [] if earlier is None else [earlier]
    return pl.pallas_call(
        body,
        in_specs=[pl.BlockSpec(memory_space=pltpu.VMEM)] * 4
        + [pl.BlockSpec(memory_space=pltpu.HBM)] * len(more),
        out_specs=pl.BlockSpec(memory_space=pltpu.HBM),
        out_shape=jax.ShapeDtypeStruct(shape, jnp.float32),
        input_output_aliases={4: 0} if more else {},
        scratch_shapes=[
            pltpu.VMEM((len(blocks), HALF, WIDE), jnp.float32),
            pltpu.SemaphoreType.DMA((len(blocks),)),
        ],
        compiler_params=pltpu.CompilerParams(vmem_limit_bytes=VMEM_LIMIT),
    )(in_vmem(base_blocks), *[in_vmem(u) for u in updates], *more)


def next_momentum(old, returned, shape):
    rows = 2 * HALF

    def body(old_buf, stayed, came, out_hbm, out_buf, out_sem):
        xh, c = lax.axis_index("xh"), lax.axis_index("c")
        copies = []
        for dx in range(2):
            for dc in range(2):
                row = pl.multiple_of(rows * (2 * (xh ^ dx) + (c ^ dc)), rows)
                average = came[dx] if dc else stayed[dx, 0]
                out_buf[dx, dc] = MOMENTUM_COEF * old_buf[dx, dc] + average.astype(jnp.float32)
                copy = pltpu.make_async_copy(
                    out_buf.at[dx, dc], out_hbm.at[pl.ds(row, rows)], out_sem.at[dx, dc]
                )
                copy.start()
                copies.append(copy)
        for copy in copies:
            copy.wait()

    return pl.pallas_call(
        body,
        in_specs=[pl.BlockSpec(memory_space=pltpu.VMEM)] * 3,
        out_specs=pl.BlockSpec(memory_space=pltpu.HBM),
        out_shape=jax.ShapeDtypeStruct(shape, jnp.float32),
        scratch_shapes=[pltpu.VMEM(old.shape, jnp.float32), pltpu.SemaphoreType.DMA((2, 2))],
        compiler_params=pltpu.CompilerParams(vmem_limit_bytes=VMEM_LIMIT),
        name="momentum",
    )(in_vmem(old), *[in_vmem(v) for v in returned])


def momentum_to_holders(stays, leaves):
    holder = {(column_plane(r, z, c), z, c): r for r in range(8) for z in range(8) for c in range(2)}
    owner = {(r, column_plane(r, z, c), c): z for r in range(8) for z in range(8) for c in range(2)}
    other = send(leaves, lambda r, z, xh, c: (r, z, xh, 1 - c))
    moved = [
        send(
            jnp.stack([stays[dx], other[dx]]), lambda r, z, xh, c: (holder[z, r, c], z, xh ^ dx, c)
        )
        for dx in range(2)
    ]
    m = send(jnp.stack(moved), lambda r, z, xh, c: (r, owner[r, z, c], xh, c))
    return m.reshape(8, HALF, WIDE)


def average_to_owners(average):
    average = average.reshape(2, 2, 2 * HALF, WIDE)
    other = send(average[1], lambda r, z, xh, c: (r, z, 1 - xh, c))
    average = jnp.stack([average[0], other])
    average = send(average, lambda r, z, xh, c: (z, column_plane(r, z, c), xh, c))
    other = send(average[:, 1], lambda r, z, xh, c: (r, z, xh, 1 - c))
    return average, other


def f32(value):
    return value.astype(jnp.float32)


def b16(value):
    return value.astype(jnp.bfloat16)


def per_device(local_weights, base_weights, momentum):
    return outer_step(local_weights[0], base_weights, momentum)


def outer_step(local, base, momentum):
    count = lax.axis_size(R)
    *sends, base_1, stays, leaves, old = deltas(local, base, momentum, 1)
    held = momentum_to_holders(stays, leaves)
    first = [exchange(sends[p], order[0]) for p, (order, _) in enumerate(PARTS)]
    *kept, base_0 = deltas(local, base, None, 0)
    second, third, averages, updates = [], [], [], []
    for p, (order, units) in enumerate(PARTS):
        out = b16(f32(kept[p][2:]) + f32(first[p][2:]))
        second.append(exchange(out, order[1]))
    for p, (order, units) in enumerate(PARTS):
        out = b16(f32(kept[p][1]) + f32(first[p][1]) + f32(second[p][1]))
        third.append(exchange(out, order[2]))
    for p, (order, units) in enumerate(PARTS):
        total = f32(kept[p][0]) + f32(first[p][0]) + f32(second[p][0]) + f32(third[p])
        average = total * (1.0 / count)
        new = MOMENTUM_COEF * f32(held[units[0] : units[-1] + 1]) + average
        averages.append(b16(average))
        updates.append(b16(LEARN_RATE * (average + MOMENTUM_COEF * new))[None])
    returned = average_to_owners(jnp.concatenate(averages))
    for step in (2, 1):
        for p, (order, units) in enumerate(PARTS):
            more = exchange(updates[p], order[step])
            updates[p] = jnp.concatenate([updates[p], more])
    last = [exchange(updates[p], order[0]) for p, (order, _) in enumerate(PARTS)]
    new_weights = apply_updates(base_0, updates, 0, base.shape, None)
    new_momentum = next_momentum(old, returned, momentum.shape)
    new_weights = apply_updates(base_1, last, 1, base.shape, new_weights)
    return new_weights, new_momentum


def solution(mesh):
    finer = Mesh(mesh.devices.reshape(4, 2, 8, 2, 2), EVERY)
    in_specs = (P(R, FSDP, None), P(FSDP, None), P(R, FSDP))
    out_specs = (P(FSDP, None), P(R, FSDP))
    return jax.shard_map(per_device, mesh=finer, in_specs=in_specs, out_specs=out_specs, check_vma=False)
```
